32 devices in a mesh: samp: 4 (over x, core), var: 8 (over z, y).
Axes of the slice: x: 2, y: 2, z: 4, core: 2. Of those that a mesh axis runs over, the one named last changes fastest.
Arguments:
- phenotype: bfloat16 [8192, 256], P(('samp', 'var')), may hold values from -1500 to 1500
- inverse_blocks: float32 [32, 256, 256], P(('samp', 'var')), may hold values from -1 to 2, as said below
- bin_sizes: int32 [4, 8], P('samp', 'var'), may hold values from 128 to 256, as said below
- slot_of: int32 [6144], P('samp'), may hold values from 0 to 2047, as said below
- dosages: bfloat16 [6144, 8192], P('samp', 'var'), may hold values from 0 to 2
Outputs:
- z_scores: float32 [8192, 256], P('var', 'samp')
The draws below stay inside these ranges and needn't reach their ends.
Inputs may be any that keep to these rules, and one draw needn't show every extreme that they name: `bin_sizes`: within each row (one sample shard) the sizes sum to 192 times the row's length, and at least one bin is full. `slot_of`: within each sample shard the samples occupy exactly the live slots: slot v * 256 + r with r < bin_sizes of bin v, each once. `inverse_blocks`: each block is symmetric positive definite.
All inputs are finite; a program needn't handle non-finite values.
Results may differ from the reference program's by a relative error of at most 0.0041.
Values may be sent and summed in bfloat16 or wider, within the bound.
No kernel may reach another device: no remote copies, remote signals or barrier semaphores. Data moves between devices by JAX's collectives and lax.ppermute only.
A program may use at most 128 MiB of HBM per device.

```python
import math
import jax
import jax.numpy as jnp
from jax import lax

B = 256
P_SIZE = 256
LIVE_DEV = 192
SHARD_SAMPLES = 1536
SAMPLES = 6144
M = 8192
NBIN = 32
N_SAMP = 4
N_VAR = 8


def shard_layout(key):
    spare = B - LIVE_DEV
    base_key = jax.random.fold_in(key, 101)
    key_order, key_amount, key_perm = jax.random.split(base_key, 3)
    bin_order = jax.vmap(lambda one_key: jax.random.permutation(one_key, N_VAR))(jax.random.split(key_order, N_SAMP)).astype(jnp.int32)
    amounts = jax.random.randint(key_amount, (N_SAMP, N_VAR // 2), 0, spare + 1).astype(jnp.int32)
    amounts = amounts.at[:, 0].set(spare)
    signed = jnp.stack([amounts, -amounts], axis=2).reshape(N_SAMP, N_VAR)
    deficit_pos = spare + signed
    shard_rows = jnp.arange(N_SAMP, dtype=jnp.int32)[:, None]
    deficits = jnp.zeros((N_SAMP, N_VAR), jnp.int32).at[shard_rows, bin_order].set(deficit_pos)
    bin_fill = (B - deficits).astype(jnp.int32)
    counter = jnp.arange(SHARD_SAMPLES, dtype=jnp.int32)

    def shard_slots(fill_row, one_key):
        bin_ends = jnp.cumsum(fill_row).astype(jnp.int32)
        bin_index = jnp.sum((counter[:, None] >= bin_ends[None, :]).astype(jnp.int32), axis=1)
        bin_starts = bin_ends - fill_row
        live_slots = bin_index * B + counter - bin_starts[bin_index]
        return live_slots[jax.random.permutation(one_key, SHARD_SAMPLES)].astype(jnp.int32)
    slots = jax.vmap(shard_slots)(bin_fill, jax.random.split(key_perm, N_SAMP)).reshape(SAMPLES)
    return (bin_fill, slots)


def draw_bin_sizes(key, part):
    return shard_layout(key)[0]


def draw_slot_of(key, part):
    return shard_layout(key)[1]


def draw_phenotype(key, part):
    key_a, key_b, key_c = jax.random.split(jax.random.fold_in(key, 7), 3)
    row_total = B * NBIN
    base_draw = jax.random.normal(key_a, (row_total, P_SIZE), jnp.float32)
    base_draw = jnp.clip(base_draw, -5.0, 5.0)
    row_scale = jnp.exp(jax.random.uniform(key_b, (row_total, 1), jnp.float32, 0.0, math.log(10.0)))
    trait_scale = jnp.exp(jax.random.uniform(key_c, (1, P_SIZE), jnp.float32, 0.0, math.log(10.0)))
    rising = 3.0 ** (jnp.arange(row_total, dtype=jnp.float32) / row_total)[:, None]
    return (base_draw * row_scale * trait_scale * rising).astype(jnp.bfloat16)


def draw_inverse_blocks(key, part):
    key_a, key_b = jax.random.split(jax.random.fold_in(key, 11), 2)
    spread = 0.5 / math.sqrt(B)
    raw_draw = jnp.clip(jax.random.normal(key_a, (NBIN, B, B), jnp.float32), -1.73, 1.73) * spread
    symmetric = 0.5 * (raw_draw + jnp.swapaxes(raw_draw, 1, 2))
    identity = jnp.eye(B, dtype=jnp.float32)[None, :, :]
    diagonal = 1.0 + jax.random.uniform(key_b, (NBIN, B, 1), jnp.float32, 0.0, 1.0)
    return symmetric * (1.0 - identity) + diagonal * identity


def block_levels(own_key, extent, shards, smallest, largest):
    def one(dim, blocks):
        draws = jax.random.uniform(jax.random.fold_in(jax.random.fold_in(own_key, 6), dim), (blocks,), jnp.float32, smallest / len(shards), largest / len(shards))
        return jnp.repeat(jnp.exp(draws), extent[dim] // blocks).reshape((-1,) + (1,) * (len(extent) - dim - 1))

    factor_of = one(*shards[0])
    for cut in shards[1:]:
        factor_of = factor_of * one(*cut)
    return factor_of


def setup_inputs(seed: int = 0) -> dict:
    splits = jax.random.split(jax.random.key(seed), 6)
    phenotype = draw_phenotype(jax.random.fold_in(splits[5], 71), 0)
    inverse_blocks = draw_inverse_blocks(jax.random.fold_in(splits[5], 71), 0)
    bin_sizes = draw_bin_sizes(jax.random.fold_in(splits[5], 71), 0)
    slot_of = draw_slot_of(jax.random.fold_in(splits[5], 71), 0)
    dosages = jnp.clip(2.0 * jax.random.uniform(splits[4], (SAMPLES, M), jnp.float32) ** block_levels(splits[4], (SAMPLES, M), ((0, 4), (1, 8)), -0.2, 0.2), 0.0, 2.0).astype(jnp.bfloat16)
    return dict(phenotype=phenotype, inverse_blocks=inverse_blocks, bin_sizes=bin_sizes, slot_of=slot_of, dosages=dosages)


epsilon = 1e-06

def reference(phenotype, inverse_blocks, bin_sizes, slot_of, dosages):
    bin_count = inverse_blocks.shape[0]
    bin_fill = bin_sizes.reshape(bin_count)
    position = jnp.arange(B, dtype=jnp.int32)
    live_mask = (position[None, :] < bin_fill[:, None]).astype(jnp.float32)
    masked_pheno = phenotype.astype(jnp.float32).reshape(bin_count, B, P_SIZE) * live_mask[:, :, None]
    whitened = jnp.einsum('bij,bjp->bip', inverse_blocks, masked_pheno, precision=lax.Precision.HIGHEST) * live_mask[:, :, None]
    trait_scale = lax.optimization_barrier(jnp.sum(masked_pheno * whitened, axis=(0, 1)))
    white_rows = whitened.astype(jnp.bfloat16).reshape(N_SAMP, N_VAR * B, P_SIZE)
    slot_weight = jnp.diagonal(inverse_blocks, axis1=1, axis2=2).astype(jnp.bfloat16).reshape(N_SAMP, N_VAR * B)
    shard_slots = slot_of.reshape(N_SAMP, SHARD_SAMPLES)
    shard_rows = dosages.reshape(N_SAMP, SHARD_SAMPLES, M)
    scores = jnp.zeros((M, P_SIZE), jnp.float32)
    variance = jnp.zeros((M,), jnp.float32)
    for shard in range(N_SAMP):
        picked = jnp.take(white_rows[shard], shard_slots[shard], axis=0)
        scores = scores + lax.dot_general(shard_rows[shard], picked, (((0,), (0,)), ((), ())), preferred_element_type=jnp.float32)
        sample_weight = jnp.take(slot_weight[shard], shard_slots[shard]).astype(jnp.float32)
        squares = shard_rows[shard].astype(jnp.float32) ** 2
        variance = variance + jnp.dot(sample_weight, squares, precision=lax.Precision.HIGHEST)
    return scores / jnp.sqrt(variance[:, None] * trait_scale[None, :] / SAMPLES + epsilon)
```

```python
import functools
import math

import jax
import jax.numpy as jnp
from jax import lax
from jax.experimental import pallas as pl
from jax.experimental.pallas import tpu as pltpu
from jax.sharding import PartitionSpec as P

epsilon = 1e-06
F32 = jnp.float32
BF16 = jnp.bfloat16
LANES = 128
EXTRA = 16

VMEM = pl.BlockSpec(memory_space=pltpu.VMEM)
SMEM = pl.BlockSpec(memory_space=pltpu.SMEM)


def split3(value):
    high = value.astype(BF16)
    rest = value - high.astype(F32)
    mid = rest.astype(BF16)
    low = (rest - mid.astype(F32)).astype(BF16)
    return high, mid, low


def join3(high, mid, low):
    return (low.astype(F32) + mid.astype(F32)) + high.astype(F32)


def whiten_kernel(size_ref, pheno_ref, inverse_ref, out_ref):
    width, traits = pheno_ref.shape
    live = lax.broadcasted_iota(jnp.int32, (width, traits), 0) < size_ref[0, 0]
    masked = jnp.where(live, pheno_ref[...].astype(F32), 0.0)
    masked_low = masked.astype(BF16)
    inverse = inverse_ref[0]
    high, mid, low = split3(inverse)
    dot = functools.partial(jnp.dot, preferred_element_type=F32)
    whitened = dot(high, masked_low) + (dot(mid, masked_low) + dot(low, masked_low))
    whitened = jnp.where(live, whitened, 0.0)
    out_ref[:traits, :] = whitened.T.astype(BF16)
    form = jnp.sum(masked * whitened, axis=0, keepdims=True)
    square = lax.broadcasted_iota(jnp.int32, (width, width), 0) == lax.broadcasted_iota(
        jnp.int32, (width, width), 1
    )
    weight = jnp.sum(jnp.where(square, inverse, 0.0), axis=0, keepdims=True)
    high, mid, low = split3(form)
    row = lax.broadcasted_iota(jnp.int32, (EXTRA, width), 0)
    extra = jnp.where(row == 0, weight, 0.0)
    extra = jnp.where(row == 1, high.astype(F32), extra)
    extra = jnp.where(row == 2, mid.astype(F32), extra)
    extra = jnp.where(row == 3, low.astype(F32), extra)
    out_ref[traits:, :] = extra.astype(BF16)


def whiten(bin_sizes, phenotype, inverse_blocks):
    width, traits = phenotype.shape
    return pl.pallas_call(
        whiten_kernel,
        out_shape=jax.ShapeDtypeStruct((traits + EXTRA, width), BF16),
        in_specs=[SMEM, VMEM, VMEM],
        out_specs=VMEM,
        name="whiten",
    )(bin_sizes, phenotype, inverse_blocks)


def arrange_kernel(slot_ref, dosage_ref, out_ref, select_ref):
    rows = out_ref.shape[0]

    @pl.when(pl.program_id(1) == 0)
    def _():
        first = pl.program_id(0) * rows
        step = 256
        for start in range(0, rows, step):
            index = lax.broadcasted_iota(jnp.int32, (step, select_ref.shape[1]), 0)
            hit = index + (first + start) == slot_ref[...]
            select_ref[start : start + step, :] = jnp.where(hit, 1.0, 0.0).astype(BF16)

    out_ref[...] = jnp.dot(
        select_ref[...], dosage_ref[...], preferred_element_type=F32
    ).astype(BF16)


def arrange(slots, dosages, slot_count):
    samples, variants = dosages.shape
    rows = slot_count
    while rows * samples * 2 > 2**24:
        rows //= 2
    columns = 256
    return pl.pallas_call(
        arrange_kernel,
        out_shape=jax.ShapeDtypeStruct((slot_count, variants), BF16),
        grid=(slot_count // rows, variants // columns),
        in_specs=[
            pl.BlockSpec((1, samples), lambda i, j: (0, 0)),
            pl.BlockSpec((samples, columns), lambda i, j: (0, j)),
        ],
        out_specs=pl.BlockSpec((rows, columns), lambda i, j: (i, j)),
        scratch_shapes=[pltpu.VMEM((rows, samples), BF16)],
        cost_estimate=pl.CostEstimate(
            flops=2 * slot_count * samples * variants,
            bytes_accessed=2 * variants * (samples + slot_count),
            transcendentals=0,
        ),
        name="arrange",
    )(slots, dosages)


def accumulate(blocks, dosage_ref, first, score_ref, extra_ref, start):
    traits = score_ref.shape[0]
    width = blocks[0].shape[1]
    variants = dosage_ref.shape[1]
    dot = functools.partial(jnp.dot, preferred_element_type=F32)
    step = 256
    for column in range(0, variants, step):
        columns = slice(column, column + step)
        score = None if start else score_ref[:, columns]
        variance = None if start else extra_ref[:EXTRA, columns]
        for i, block in enumerate(blocks):
            rows = slice((first + i) * width, (first + i + 1) * width)
            dosage = dosage_ref[rows, columns]
            part = dot(block[:traits, :], dosage)
            score = part if score is None else score + part
            wide = dosage.astype(F32)
            square = wide * wide
            high = square.astype(BF16)
            low = (square - high.astype(F32)).astype(BF16)
            weight = block[traits:, :]
            part = dot(weight, high) + dot(weight, low)
            variance = part if variance is None else variance + part
        score_ref[:, columns] = score
        extra_ref[:EXTRA, columns] = variance
    form = None if start else extra_ref[EXTRA : EXTRA + 1, :width]
    for block in blocks:
        tail = block[traits:, :].astype(F32)
        part = (tail[3:4, :] + tail[2:3, :]) + tail[1:2, :]
        form = part if form is None else form + part
    extra_ref[EXTRA : EXTRA + 1, :width] = form


def score_first_kernel(count, *refs):
    blocks, dosage_ref, score_ref, extra_ref = refs[:count], *refs[count:]
    accumulate(blocks, dosage_ref, 0, score_ref, extra_ref, True)


def score_first(blocks, arranged, traits):
    variants = arranged.shape[1]
    count = len(blocks)
    width = blocks[0].shape[1]
    return pl.pallas_call(
        functools.partial(score_first_kernel, count),
        out_shape=(
            jax.ShapeDtypeStruct((traits, variants), F32),
            jax.ShapeDtypeStruct((EXTRA + 8, variants), F32),
        ),
        in_specs=[VMEM] * (count + 1),
        out_specs=(VMEM, VMEM),
        cost_estimate=pl.CostEstimate(
            flops=4 * count * width * traits * variants,
            bytes_accessed=4 * count * width * variants,
            transcendentals=0,
        ),
        name="score_first",
    )(*blocks, arranged)


def put_rows(ref, where, base, value):
    height = value.shape[0]
    for i in range(value.shape[1] // LANES):
        ref[where, base + i * height : base + (i + 1) * height, :] = value[
            :, i * LANES : (i + 1) * LANES
        ]


def pack_extra(extra, traits):
    variants = extra.shape[1]
    rows = [extra[0:1, i * LANES : (i + 1) * LANES] for i in range(variants // LANES)]
    rows += [
        extra[EXTRA : EXTRA + 1, i * LANES : (i + 1) * LANES]
        for i in range(traits // LANES)
    ]
    pad = -len(rows) % EXTRA
    if pad:
        rows.append(jnp.zeros((pad, LANES), F32))
    return jnp.concatenate(rows, axis=0)


def extra_rows(traits, variants):
    return -(-(traits // LANES + variants // LANES) // EXTRA) * EXTRA


def put_extra(ref, where, base, packed):
    rows = packed.shape[0]
    for i, part in enumerate(split3(packed)):
        ref[where, base + i * rows : base + (i + 1) * rows, :] = part


def get_extra(value, base, rows):
    parts = [value[base + i * rows : base + (i + 1) * rows, :] for i in range(3)]
    return join3(*parts)


def score_last_kernel(count, first, chips, cores, *refs):
    core_ref = refs[0]
    blocks = refs[1 : count + 1]
    (
        dosage_ref,
        score_in,
        extra_in,
        send_ref,
        keep_ref,
        extra_keep,
        score_ref,
        extra_ref,
    ) = refs[count + 1 :]
    score_ref[...] = score_in[...]
    extra_ref[...] = extra_in[...]
    accumulate(blocks, dosage_ref, first, score_ref, extra_ref, False)
    traits, variants = score_ref.shape
    share = traits // (chips * cores)
    core = core_ref[0]
    packed = pack_extra(extra_ref[...], traits)
    extra_keep[...] = packed
    body = share * variants // LANES
    for chip in range(chips):
        own = pl.multiple_of((chip * cores + core) * share, share)
        keep_ref[chip * share : (chip + 1) * share, :] = score_ref[pl.ds(own, share), :]
    for hop in range(1, cores):
        other = lax.rem(core + hop, cores)
        for chip in range(chips):
            start = pl.multiple_of((chip * cores + other) * share, share)
            put_rows(
                send_ref,
                hop - 1,
                chip * body,
                score_ref[pl.ds(start, share), :].astype(BF16),
            )
        put_extra(send_ref, hop - 1, chips * body, packed)


def score_last(core, blocks, first, arranged, score, extra, chips, cores):
    traits, variants = score.shape
    count = len(blocks)
    share = traits // (chips * cores)
    rows = extra_rows(traits, variants)
    body = share * variants // LANES
    return pl.pallas_call(
        functools.partial(score_last_kernel, count, first, chips, cores),
        out_shape=(
            jax.ShapeDtypeStruct((cores - 1, chips * body + 3 * rows, LANES), BF16),
            jax.ShapeDtypeStruct((chips * share, variants), F32),
            jax.ShapeDtypeStruct((rows, LANES), F32),
        ),
        in_specs=[SMEM] + [VMEM] * (count + 3),
        out_specs=(VMEM, VMEM, VMEM),
        scratch_shapes=[
            pltpu.VMEM((traits, variants), F32),
            pltpu.VMEM(extra.shape, F32),
        ],
        name="score_last",
    )(core, *blocks, arranged, score, extra)


def middle_kernel(hops, chips, share, *refs):
    chip_ref, keep_ref, extra_ref = refs[:3]
    got = refs[3 : 3 + hops]
    send_ref, own_ref, extra_out = refs[3 + hops :]
    variants = keep_ref.shape[1]
    body = share * variants // LANES
    rows = extra_ref.shape[0]
    me = chip_ref[0]
    packed = extra_ref[...]
    for one in got:
        packed = packed + get_extra(one, chips * body, rows)
    extra_out[...] = packed
    for hop in range(chips):
        chip = lax.rem(me + hop, chips)
        here = pl.multiple_of(chip * share, share)
        for i in range(variants // LANES):
            lanes = slice(i * LANES, (i + 1) * LANES)
            there = pl.multiple_of(chip * body + i * share, share)
            total = keep_ref[pl.ds(here, share), lanes]
            for one in got:
                total = total + one[pl.ds(there, share), :].astype(F32)
            if hop == 0:
                own_ref[:, lanes] = total
            else:
                send_ref[hop - 1, i * share : (i + 1) * share, :] = total.astype(BF16)
        if hop:
            put_extra(send_ref, hop - 1, body, packed)


def middle(chip, keep, extra, got, chips, share):
    variants = keep.shape[1]
    body = share * variants // LANES
    rows = extra.shape[0]
    return pl.pallas_call(
        functools.partial(middle_kernel, len(got), chips, share),
        out_shape=(
            jax.ShapeDtypeStruct((max(chips - 1, 1), body + 3 * rows, LANES), BF16),
            jax.ShapeDtypeStruct((share, variants), F32),
            jax.ShapeDtypeStruct((rows, LANES), F32),
        ),
        in_specs=[SMEM] + [VMEM] * (2 + len(got)),
        out_specs=(VMEM, VMEM, VMEM),
        name="middle",
    )(chip, keep, extra, *got)


def final_kernel(hops, traits, samples, *refs):
    samp_ref, own_ref, extra_ref = refs[:3]
    got = refs[3 : 3 + hops]
    out_ref = refs[3 + hops]
    share, variants = own_ref.shape
    body = share * variants // LANES
    rows = extra_ref.shape[0]
    packed = extra_ref[...]
    for one in got:
        packed = packed + get_extra(one, body, rows)
    base = variants // LANES
    trait = samp_ref[0] * share + lax.broadcasted_iota(jnp.int32, (share, LANES), 0)
    lane = lax.broadcasted_iota(jnp.int32, (share, LANES), 1)
    form = jnp.zeros((share, LANES), F32)
    for i in range(traits // LANES):
        form = form + jnp.where(
            lane + i * LANES == trait, packed[base + i : base + i + 1, :], 0.0
        )
    form = jnp.sum(form, axis=1, keepdims=True)
    for i in range(variants // LANES):
        lanes = slice(i * LANES, (i + 1) * LANES)
        total = own_ref[:, lanes]
        for one in got:
            total = total + one[i * share : (i + 1) * share, :].astype(F32)
        scale = packed[i : i + 1, :] * form / samples + epsilon
        out_ref[lanes, :] = (total * lax.rsqrt(scale)).T


def final(samp, own, extra, got, traits, samples):
    share, variants = own.shape
    return pl.pallas_call(
        functools.partial(final_kernel, len(got), traits, samples),
        out_shape=jax.ShapeDtypeStruct((variants, share), F32),
        in_specs=[SMEM] + [VMEM] * (2 + len(got)),
        out_specs=VMEM,
        name="final",
    )(samp, own, extra, *got)


def shift(count, inner, outer_hop, inner_hop):
    outer = count // inner
    pairs = []
    for source in range(count):
        o, i = divmod(source, inner)
        pairs.append(
            (source, (o + outer_hop) % outer * inner + (i + inner_hop) % inner)
        )
    return pairs


def inner_factor(count):
    inner = 1
    while (inner * 2) ** 2 <= count and count % (inner * 2) == 0:
        inner *= 2
    return inner


def solution(mesh):
    n_samp, n_var = mesh.shape["samp"], mesh.shape["var"]
    inner = inner_factor(n_var)
    outer = n_var // inner
    cores = 2 if n_samp % 2 == 0 else 1
    chips = n_samp // cores

    def local(phenotype, inverse_blocks, bin_sizes, slot_of, dosages):
        width, traits = phenotype.shape
        samples = slot_of.shape[0]
        samp, var = lax.axis_index("samp"), lax.axis_index("var")
        own = whiten(bin_sizes, phenotype, inverse_blocks)

        of_bin, of_row = slot_of // width, slot_of % width
        hop_outer = (var // inner - of_bin // inner) % outer
        hop_inner = (var % inner - of_bin % inner) % inner
        place = hop_inner * outer + hop_outer
        slots = (place * width + of_row).reshape(1, samples)
        arranged = arrange(slots, dosages, n_var * width)

        order = sorted(range(1, outer), key=lambda k: min(k, outer - k))
        line = {0: own}
        for k in order:
            line[k] = lax.ppermute(own, "var", shift(n_var, inner, k, 0))
        side = []
        for h in range(1, inner):
            pairs = shift(n_var, inner, 0, h)
            passed = {k: lax.ppermute(line[k], "var", pairs) for k in [0] + order}
            side += [passed[k] for k in range(outer)]
        near = [line[k] for k in range(outer)]
        score, extra = score_first(near, arranged, traits)
        core = (samp % cores).reshape(1)
        chip = (samp // cores).reshape(1)
        send, keep, extra = score_last(
            core, side, outer, arranged, score, extra, chips, cores
        )
        got = [
            lax.ppermute(send[h - 1], "samp", shift(n_samp, cores, 0, h))
            for h in range(1, cores)
        ]
        share = traits // n_samp
        send, mine, extra = middle(chip, keep, extra, got, chips, share)
        got = [
            lax.ppermute(send[h - 1], "samp", shift(n_samp, cores, h, 0))
            for h in range(1, chips)
        ]
        return final(samp.reshape(1), mine, extra, got, traits, samples * n_samp)

    in_specs = (
        P(("samp", "var"), None),
        P(("samp", "var"), None, None),
        P("samp", "var"),
        P("samp"),
        P("samp", "var"),
    )
    return jax.shard_map(
        local, mesh=mesh, in_specs=in_specs, out_specs=P("var", "samp"), check_vma=False
    )
```
